128 devices in a mesh: dev: 128 (over y, x, z, core).
Axes of the slice: x: 4, y: 4, z: 4, core: 2. Of those that a mesh axis runs over, the one named last changes fastest.
Arguments:
- images: bfloat16 [1024, 768, 1536], P('dev'), may hold values from -6 to 6
- legendre: bfloat16 [128, 704, 768], P('dev'), may hold values from -0.21875 to 0.21875
- leakage: float32 [128, 3, 13, 704], P('dev'), may hold values from -1 to 1
Outputs:
- modes: float32 [128, 704, 2048], P('dev')
The draws below stay inside these ranges and needn't reach their ends.
All inputs are finite; a program needn't handle non-finite values.
Results may differ from the reference program's by a relative error of at most 0.0053.
Values may be sent and summed in bfloat16 or wider, within the bound.
No kernel may reach another device: no remote copies, remote signals or barrier semaphores. Data moves between devices by JAX's collectives and lax.ppermute only.
A program may use at most 128 MiB of HBM per device.

```python
import math
import jax
import jax.numpy as jnp
from jax import lax

NLAT = 768
NLON = 1536
DEG = 704
BAND = 6
NT = 1024
M_ORD = 128


def shard_levels(rng, extent, cuts, least, top_value):
    level = 1.0
    for axis_at, shards_of in cuts:
        draws = jax.random.uniform(jax.random.fold_in(jax.random.fold_in(rng, 6), axis_at), (shards_of,), jnp.float32, least / len(cuts), top_value / len(cuts))
        level = level * jnp.repeat(jnp.exp(draws), extent[axis_at] // shards_of).reshape((-1,) + (1,) * (len(extent) - 1 - axis_at))
    return level


def centred(rng, extent, deviation, limit, pieces=(), kind=jnp.bfloat16):
    entries = deviation * jax.random.normal(rng, extent, jnp.float32)
    if pieces:
        entries = entries * shard_levels(rng, extent, pieces, -0.22, 0.18)
    return jnp.clip(entries, -limit, limit).astype(kind)


def setup_inputs(seed: int = 0) -> dict:
    key_list = jax.random.split(jax.random.key(seed), 4)
    return {
        "images": centred(key_list[0], (NT, NLAT, NLON), 1.0, 6.0, ((0, 128),)),
        "legendre": centred(key_list[1], (M_ORD, DEG, NLAT), NLAT ** -0.5, 0.21875, ((0, 128),)),
        "leakage": centred(key_list[2], (M_ORD, 3, 2 * BAND + 1, DEG), 0.16, 1.0, ((0, 128),), jnp.float32),
    }


def lon_table(nlon, norders):
    index = jnp.arange(nlon, dtype=jnp.int32)[None, :]
    order = jnp.arange(norders, dtype=jnp.int32)[:, None]
    phase = (index * order % nlon).astype(jnp.float32)
    angle = 2.0 * math.pi * phase / nlon
    table = jnp.stack([jnp.cos(angle), -jnp.sin(angle)], axis=1) / math.sqrt(nlon)
    return table.reshape(2 * norders, nlon).astype(jnp.bfloat16)

def time_table(ntimes):
    index = jnp.arange(ntimes, dtype=jnp.int32)
    phase = (index[:, None] * index[None, :] % ntimes).astype(jnp.float32)
    angle = 2.0 * math.pi * phase / ntimes
    cosine = jnp.cos(angle)
    sine = jnp.sin(angle)
    upper = jnp.concatenate([cosine, -sine], axis=1)
    lower = jnp.concatenate([sine, cosine], axis=1)
    return (jnp.concatenate([upper, lower], axis=0) / math.sqrt(ntimes)).astype(jnp.bfloat16)

def reference(images, legendre, leakage):
    table = lon_table(NLON, M_ORD).astype(jnp.float32)

    def one_image(image):
        out = jnp.dot(table, image.astype(jnp.float32).T, preferred_element_type=jnp.float32)
        return out.astype(jnp.bfloat16)
    lon = lax.map(one_image, images)
    lon = jnp.transpose(lon.reshape(NT, M_ORD, 2, NLAT), (1, 2, 0, 3))
    wtable = time_table(NT)
    degrees = jnp.arange(DEG, dtype=jnp.int32)

    def one_order(args):
        order, table_rows, data = args
        flat = data.reshape(2 * NT, NLAT)
        coef = lax.dot_general(table_rows, flat, (((1,), (1,)), ((), ())), preferred_element_type=jnp.float32)
        coef = jnp.where((degrees >= order)[:, None], coef, jnp.float32(0.0)).astype(jnp.bfloat16)
        return jnp.dot(coef, wtable, preferred_element_type=jnp.float32)
    orders = jnp.arange(M_ORD, dtype=jnp.int32)
    spectra = lax.map(one_order, (orders, legendre, lon))
    padded = jnp.pad(spectra, ((1, 1), (BAND, BAND), (0, 0)))

    def one_mode(args):
        order, coeffs = args
        rows = lax.dynamic_slice(padded, (order.astype(jnp.int32), jnp.int32(0), jnp.int32(0)), (3, DEG + 2 * BAND, 2 * NT))
        total = jnp.zeros((DEG, 2 * NT), jnp.float32)
        for shift in range(3):
            for offset in range(2 * BAND + 1):
                total = total + coeffs[shift, offset][:, None] * rows[shift, offset:offset + DEG]
        return jnp.where((degrees >= order)[:, None], total, jnp.float32(0.0))
    return lax.map(one_mode, (orders, leakage))
```

```python
import math

import jax
import jax.numpy as jnp
import numpy as np
from jax import lax
from jax.experimental import pallas as pl
from jax.experimental.pallas import tpu as pltpu
from jax.sharding import PartitionSpec as P

BAND = 6
F32 = jnp.float32
BF16 = jnp.bfloat16
MIB = 1 << 20
GROUPS = 2
CHUNKS = ((0, 0, 1024), (1, 0, 512), (1, 512, 512))
NT_DIMS = (((1,), (1,)), ((), ()))


def lon_table(nlon, norders):
    phase = (np.arange(nlon)[:, None] * np.arange(norders)[None, :]) % nlon
    angle = 2.0 * math.pi * phase / nlon
    table = np.concatenate([np.cos(angle), -np.sin(angle)], axis=1) / math.sqrt(nlon)
    return table.astype(BF16)


def time_factors(nsrc, tloc, group):
    ntimes = nsrc * tloc
    per = tloc // GROUPS
    slow = 2.0 * math.pi * ((np.arange(nsrc)[:, None] * np.arange(128)[None, :]) % nsrc) / nsrc
    local = group * per + np.arange(per)
    fast = 2.0 * math.pi * ((local[:, None] * np.arange(ntimes)[None, :]) % ntimes) / ntimes
    slow = np.stack([np.cos(slow), np.sin(slow)]) / math.sqrt(ntimes)
    plain = np.stack([np.cos(fast), np.sin(fast)], axis=1).reshape(2 * per, ntimes)
    turned = np.stack([-np.sin(fast), np.cos(fast)], axis=1).reshape(2 * per, ntimes)
    return slow.astype(np.float32), np.stack([plain, turned]).astype(np.float32)


def transform_images(images, norders, group, after):
    tloc, nlat, nlon = images.shape
    per = tloc // GROUPS
    tile, some = 256, 8
    rows = 2 * norders

    def kernel(table_ref, image_ref, *refs):
        out_ref, turned_ref = refs[-2:]
        flat = image_ref[...].reshape(per * tile, nlon)
        part = jnp.dot(flat, table_ref[...], preferred_element_type=F32)
        for t in range(per):
            turned_ref[2 * t : 2 * t + 2] = part[t * tile : (t + 1) * tile].T.reshape(2, norders, tile)
        for i in range(0, norders, some):
            swapped = jnp.swapaxes(turned_ref[:, i : i + some, :], 0, 1)
            out_ref[i : i + some] = swapped.astype(BF16)

    return pl.pallas_call(
        kernel,
        grid=(nlat // tile,),
        in_specs=[
            pl.BlockSpec((nlon, rows), lambda j: (0, 0)),
            pl.BlockSpec((per, tile, nlon), lambda j: (group, j, 0)),
        ]
        + [pl.BlockSpec(memory_space=pltpu.HBM)] * len(after),
        out_specs=pl.BlockSpec((norders, 2 * per, tile), lambda j: (0, 0, j)),
        out_shape=jax.ShapeDtypeStruct((norders, 2 * per, nlat), BF16),
        scratch_shapes=[pltpu.VMEM((2 * per, norders, tile), F32)],
        compiler_params=pltpu.CompilerParams(vmem_limit_bytes=60 * MIB),
        cost_estimate=pl.CostEstimate(
            flops=2 * rows * per * nlat * nlon, bytes_accessed=images.size * 2, transcendentals=0
        ),
        name="lon",
    )(jnp.asarray(lon_table(nlon, norders)), images, *after)


def time_matrix(nsrc, tloc, group, first, count, after):
    ntimes = nsrc * tloc
    slow, fast = time_factors(nsrc, tloc, group)
    rows = 2 * tloc // GROUPS
    per = 32
    lanes = 128
    start = first // rows // per

    def kernel(slow_ref, fast_ref, after_ref, out_ref, token_ref):
        token_ref[...] = jnp.zeros(token_ref.shape, F32)

        def sources(s, carry):
            a = [slow_ref[0, pl.ds(2 * s + u, 1), :] for u in range(2)]
            b = [slow_ref[1, pl.ds(2 * s + u, 1), :] for u in range(2)]
            here = pl.ds(pl.multiple_of(s * 2 * rows, 2 * rows), 2 * rows)
            for f in range(ntimes // lanes):
                cols = slice(f * lanes, (f + 1) * lanes)
                more = slice(ntimes + f * lanes, ntimes + (f + 1) * lanes)
                plain = fast_ref[0, :, cols]
                turned = fast_ref[1, :, cols]
                left = [a[u] * plain + b[u] * turned for u in range(2)]
                right = [a[u] * turned - b[u] * plain for u in range(2)]
                out_ref[here, cols] = jnp.concatenate(left, axis=0).astype(BF16)
                out_ref[here, more] = jnp.concatenate(right, axis=0).astype(BF16)
            return carry

        lax.fori_loop(0, per // 2, sources, 0)

    return pl.pallas_call(
        kernel,
        grid=(count // rows // per,),
        in_specs=[
            pl.BlockSpec((2, per, lanes), lambda i: (0, start + i, 0)),
            pl.BlockSpec((2, rows, ntimes), lambda i: (0, 0, 0)),
            pl.BlockSpec(memory_space=pltpu.HBM),
        ],
        out_specs=[
            pl.BlockSpec((per * rows, 2 * ntimes), lambda i: (i, 0)),
            pl.BlockSpec((8, lanes), lambda i: (0, 0)),
        ],
        out_shape=[
            jax.ShapeDtypeStruct((count, 2 * ntimes), BF16),
            jax.ShapeDtypeStruct((8, lanes), F32),
        ],
        compiler_params=pltpu.CompilerParams(vmem_limit_bytes=60 * MIB),
        cost_estimate=pl.CostEstimate(
            flops=100_000_000, bytes_accessed=4 * ntimes * count, transcendentals=0
        ),
        name="time_matrix",
    )(jnp.asarray(slow), jnp.asarray(fast), after)


def windows(degrees, tile, reach):
    size = tile + 2 * reach
    return size, [min(max(i * tile - reach, 0), degrees - size) for i in range(degrees // tile)]


def band_matrices(leakage, order, tile, reach, after):
    shifts, width, degrees = leakage.shape
    size, starts = windows(degrees, tile, reach)
    tiles = degrees // tile
    columns = jnp.transpose(leakage, (0, 2, 1))

    def kernel(order_ref, columns_ref, after_ref, out_ref, token_ref):
        token_ref[...] = jnp.zeros(token_ref.shape, F32)
        for i in range(tiles):
            row = lax.broadcasted_iota(jnp.int32, (tile, size), 0)
            col = lax.broadcasted_iota(jnp.int32, (tile, size), 1)
            offset = col - row + (starts[i] - i * tile + BAND)
            offset = jnp.where(row + i * tile >= order_ref[0], offset, -1)
            odd = lax.rem(order_ref[0], 2)
            for d, shift in enumerate((2 - 2 * odd, 1, 2 * odd)):
                values = columns_ref[shift, i * tile : (i + 1) * tile, :]
                total = jnp.zeros((tile, size), F32)
                for k in range(width):
                    total = jnp.where(offset == k, values[:, k : k + 1], total)
                out_ref[d, i] = total.astype(BF16)

    return pl.pallas_call(
        kernel,
        in_specs=[
            pl.BlockSpec(memory_space=pltpu.SMEM),
            pl.BlockSpec(memory_space=pltpu.VMEM),
            pl.BlockSpec(memory_space=pltpu.HBM),
        ],
        out_specs=[pl.BlockSpec(memory_space=pltpu.VMEM)] * 2,
        out_shape=[
            jax.ShapeDtypeStruct((shifts, tiles, tile, size), BF16),
            jax.ShapeDtypeStruct((8, 128), F32),
        ],
        compiler_params=pltpu.CompilerParams(vmem_limit_bytes=60 * MIB),
        cost_estimate=pl.CostEstimate(
            flops=100_000_000, bytes_accessed=2_000_000, transcendentals=0
        ),
        name="bands",
    )(order.reshape(1), columns, after)


def coefficients(legendre, data, order, first, count, after):
    degrees, nlat = legendre.shape
    tile = 256

    def kernel(order_ref, rows_hbm, data_hbm, *refs):
        out_ref, rows_ref, data_ref, sems = refs[-4:]
        copies = [
            pltpu.make_async_copy(
                data_hbm.at[pl.ds(first + n * tile, tile)],
                data_ref.at[pl.ds(n * tile, tile)],
                sems.at[n + 1],
            )
            for n in range(count // tile)
        ]
        rows_copy = pltpu.make_async_copy(rows_hbm, rows_ref, sems.at[0])
        copies[0].start()
        rows_copy.start()
        for copy in copies[1:]:
            copy.start()
        rows_copy.wait()
        for n in range(count // tile):
            copies[n].wait()
            coef = lax.dot_general(
                rows_ref[...],
                data_ref[n * tile : (n + 1) * tile, :],
                NT_DIMS,
                preferred_element_type=F32,
            )
            degree = lax.broadcasted_iota(jnp.int32, coef.shape, 0)
            coef = jnp.where(degree >= order_ref[0], coef, 0.0)
            out_ref[:, n * tile : (n + 1) * tile] = coef.astype(BF16)

    hbm = pl.BlockSpec(memory_space=pltpu.HBM)
    anywhere = pl.BlockSpec(memory_space=pl.ANY)
    return pl.pallas_call(
        kernel,
        in_specs=[pl.BlockSpec(memory_space=pltpu.SMEM)] + [hbm] * 2 + [anywhere] * len(after),
        out_specs=pl.BlockSpec(memory_space=pltpu.VMEM),
        out_shape=jax.ShapeDtypeStruct((degrees, count), BF16),
        scratch_shapes=[
            pltpu.VMEM((degrees, nlat), BF16),
            pltpu.VMEM((count, nlat), BF16),
            pltpu.SemaphoreType.DMA((count // tile + 1,)),
        ],
        compiler_params=pltpu.CompilerParams(vmem_limit_bytes=16 * MIB),
        cost_estimate=pl.CostEstimate(
            flops=2 * degrees * nlat * count, bytes_accessed=2 * count * (nlat + degrees), transcendentals=0
        ),
        name="coef",
    )(order.reshape(1), legendre, data, *after)


def deconvolve(near, here, far, bands, wtable, partial, last):
    degrees, count = here.shape
    total = wtable.shape[1]
    shifts, tiles, tile, size = bands.shape
    _, starts = windows(degrees, tile, (size - tile) // 2)
    block, strip = 256, 512
    more = partial is not None

    def kernel(near_ref, here_ref, far_ref, bands_ref, wtable_ref, *refs):
        refs = list(refs)
        partial_ref = refs.pop(0) if more else None
        out_ref, mixed_ref = refs[:2]
        sources = (near_ref, here_ref, far_ref)
        for i in range(tiles):
            for n in range(count // strip):
                cols = slice(n * strip, (n + 1) * strip)
                acc = jnp.zeros((tile, strip), F32)
                for d in range(shifts):
                    acc += jnp.dot(
                        bands_ref[d, i],
                        sources[d][starts[i] : starts[i] + size, cols],
                        preferred_element_type=F32,
                    )
                mixed_ref[i * tile : (i + 1) * tile, cols] = acc.astype(BF16)
        copies = []
        for n in range(total // block):
            cols = slice(n * block, (n + 1) * block)
            acc = jnp.dot(
                mixed_ref[...], wtable_ref[:, cols], preferred_element_type=F32
            )
            if more:
                acc += partial_ref[:, cols]
            if not last:
                out_ref[:, cols] = acc
                continue
            stage_ref, sems = refs[2:]
            stage_ref[n] = acc
            copies.append(pltpu.make_async_copy(stage_ref.at[n], out_ref.at[:, cols], sems.at[n]))
            copies[n].start()
        for copy in copies:
            copy.wait()

    vmem = pl.BlockSpec(memory_space=pltpu.VMEM)
    scratch = [pltpu.VMEM((degrees, count), BF16)]
    inputs = [near, here, far, bands, wtable]
    if last:
        scratch += [
            pltpu.VMEM((total // block, degrees, block), F32),
            pltpu.SemaphoreType.DMA((total // block,)),
        ]
    if more:
        inputs.append(partial)
    return pl.pallas_call(
        kernel,
        in_specs=[vmem] * len(inputs),
        out_specs=pl.BlockSpec(memory_space=pltpu.HBM) if last else vmem,
        out_shape=jax.ShapeDtypeStruct((degrees, total), F32),
        scratch_shapes=scratch,
        compiler_params=pltpu.CompilerParams(vmem_limit_bytes=16 * MIB),
        cost_estimate=pl.CostEstimate(
            flops=2 * degrees * count * total, bytes_accessed=30_000_000, transcendentals=0
        ),
        name="last" if last else "deconvolve",
    )(*inputs)


def on_device(images, legendre, leakage):
    devices = lax.axis_size("dev")
    order = lax.axis_index("dev").astype(jnp.int32)
    tloc, nlat, _ = images.shape
    mates = [(i, i ^ 1) for i in range(devices)]
    across = [(i, i - 1 + 2 * (i % 2)) for i in range(1, devices - 1)]
    data, after = [], ()
    for group in range(GROUPS):
        sent = transform_images(images, devices, group, after)
        gathered = lax.all_to_all(sent, "dev", split_axis=0, concat_axis=0, tiled=True)
        data.append(gathered.reshape(-1, nlat))
        if group == 0:
            tables, after = zip(*[time_matrix(devices, tloc, *chunk, sent) for chunk in CHUNKS])
            bands, token = band_matrices(leakage[0], order, 176, 16, sent)
            after = (token, *after)
    after = ()
    parts = []
    for group, first, count in CHUNKS:
        coef = coefficients(legendre[0], data[group], order, first, count, after)
        far = lax.ppermute(coef, "dev", across)
        near = lax.ppermute(coef, "dev", mates)
        parts.append((near, coef, far))
        after = (coef,)
    partial = None
    for n, (part, wtable) in enumerate(zip(parts, tables)):
        partial = deconvolve(*part, bands, wtable, partial, n == len(CHUNKS) - 1)
    return partial[None]


def solution(mesh):
    placed = (P("dev", None, None), P("dev", None, None), P("dev", None, None, None))
    return jax.shard_map(
        on_device, mesh=mesh, in_specs=placed, out_specs=P("dev", None, None), check_vma=False
    )
```

```python
import math

import jax
import jax.numpy as jnp
import numpy as np
from jax import lax
from jax.experimental import pallas as pl
from jax.experimental.pallas import tpu as pltpu
from jax.sharding import PartitionSpec as P

BAND = 6
F32 = jnp.float32
BF16 = jnp.bfloat16
MIB = 1 << 20
ALL_VMEM = 67_000_000
GROUPS = 2
CHUNKS = ((1024,), (768, 256))
PLACES = ((0, False), (0, False), (768, True))
NT_DIMS = (((1,), (1,)), ((), ()))


def lon_table(nlon, norders):
    phase = (np.arange(nlon)[:, None] * np.arange(norders)[None, :]) % nlon
    angle = 2.0 * math.pi * phase / nlon
    table = np.concatenate([np.cos(angle), -np.sin(angle)], axis=1) / math.sqrt(nlon)
    return table.astype(BF16)


def time_factors(nsrc, tloc):
    half = nsrc * tloc // 2
    per = tloc // GROUPS
    slow = 2.0 * math.pi * ((np.arange(nsrc)[:, None] * np.arange(128)[None, :]) % nsrc) / nsrc
    fast = 2.0 * math.pi * ((np.arange(per)[:, None] * np.arange(half)[None, :]) % half) / half
    slow = np.stack([np.cos(slow), np.sin(slow)]) / math.sqrt(2 * half)
    plain = np.stack([np.cos(fast), np.sin(fast)], axis=1).reshape(2 * per, half)
    turned = np.stack([-np.sin(fast), np.cos(fast)], axis=1).reshape(2 * per, half)
    turn = math.pi * np.arange(half) / half
    turn = np.stack([np.cos(turn), np.sin(turn)])
    return [x.astype(np.float32) for x in (slow, np.stack([plain, turned]), turn)]


def transform_images(images, norders, group, after):
    tloc, nlat, nlon = images.shape
    per = tloc // GROUPS
    tile, some = 384, 8
    rows = 2 * norders

    def kernel(table_ref, image_ref, *refs):
        out_ref, turned_ref = refs[-2:]
        flat = image_ref[...].reshape(per * tile, nlon)
        part = jnp.dot(flat, table_ref[...], preferred_element_type=F32)
        for t in range(per):
            turned_ref[2 * t : 2 * t + 2] = part[t * tile : (t + 1) * tile].T.reshape(2, norders, tile)
        for i in range(0, norders, some):
            swapped = jnp.swapaxes(turned_ref[:, i : i + some, :], 0, 1)
            out_ref[i : i + some] = swapped.astype(BF16)

    return pl.pallas_call(
        kernel,
        grid=(nlat // tile,),
        in_specs=[
            pl.BlockSpec((nlon, rows), lambda j: (0, 0)),
            pl.BlockSpec((per, None, tile, nlon), lambda j: (0, group, j, 0)),
        ]
        + [pl.BlockSpec(memory_space=pltpu.HBM)] * len(after),
        out_specs=pl.BlockSpec((norders, 2 * per, tile), lambda j: (0, 0, j)),
        out_shape=jax.ShapeDtypeStruct((norders, 2 * per, nlat), BF16),
        scratch_shapes=[pltpu.VMEM((2 * per, norders, tile), F32)],
        compiler_params=pltpu.CompilerParams(vmem_limit_bytes=ALL_VMEM),
        cost_estimate=pl.CostEstimate(
            flops=2 * rows * per * nlat * nlon, bytes_accessed=images.size * 2, transcendentals=0
        ),
        name="lon",
    )(jnp.asarray(lon_table(nlon, norders)), images.reshape(per, GROUPS, nlat, nlon), *after)


def time_matrix(nsrc, tloc, after):
    ntimes = nsrc * tloc // 2
    slow, fast, _ = time_factors(nsrc, tloc)
    rows = 2 * tloc // GROUPS
    per = 32
    lanes = 128
    count = nsrc * rows

    def kernel(slow_ref, fast_ref, after_ref, out_ref, token_ref):
        token_ref[...] = jnp.zeros(token_ref.shape, F32)

        def sources(s, carry):
            a = [slow_ref[0, pl.ds(2 * s + u, 1), :] for u in range(2)]
            b = [slow_ref[1, pl.ds(2 * s + u, 1), :] for u in range(2)]
            here = pl.ds(pl.multiple_of(s * 2 * rows, 2 * rows), 2 * rows)
            for f in range(ntimes // lanes):
                cols = slice(f * lanes, (f + 1) * lanes)
                more = slice(ntimes + f * lanes, ntimes + (f + 1) * lanes)
                plain = fast_ref[0, :, cols]
                turned = fast_ref[1, :, cols]
                left = [a[u] * plain + b[u] * turned for u in range(2)]
                right = [a[u] * turned - b[u] * plain for u in range(2)]
                out_ref[here, cols] = jnp.concatenate(left, axis=0).astype(BF16)
                out_ref[here, more] = jnp.concatenate(right, axis=0).astype(BF16)
            return carry

        lax.fori_loop(0, per // 2, sources, 0)

    return pl.pallas_call(
        kernel,
        grid=(count // rows // per,),
        in_specs=[
            pl.BlockSpec((2, per, lanes), lambda i: (0, i, 0)),
            pl.BlockSpec((2, rows, ntimes), lambda i: (0, 0, 0)),
            pl.BlockSpec(memory_space=pltpu.HBM),
        ],
        out_specs=[
            pl.BlockSpec((per * rows, 2 * ntimes), lambda i: (i, 0)),
            pl.BlockSpec((8, lanes), lambda i: (0, 0)),
        ],
        out_shape=[
            jax.ShapeDtypeStruct((count, 2 * ntimes), BF16),
            jax.ShapeDtypeStruct((8, lanes), F32),
        ],
        compiler_params=pltpu.CompilerParams(vmem_limit_bytes=ALL_VMEM),
        cost_estimate=pl.CostEstimate(
            flops=100_000_000, bytes_accessed=4 * ntimes * count, transcendentals=0
        ),
        name="time_matrix",
    )(jnp.asarray(slow), jnp.asarray(fast), after)


def windows(degrees, tile, reach):
    size = tile + 2 * reach
    return size, [min(max(i * tile - reach, 0), degrees - size) for i in range(degrees // tile)]


def band_matrices(leakage, order, tile, reach, after):
    shifts, width, degrees = leakage.shape
    size, starts = windows(degrees, tile, reach)
    tiles = degrees // tile
    columns = jnp.transpose(leakage, (0, 2, 1))

    def kernel(order_ref, columns_ref, after_ref, out_ref, token_ref):
        token_ref[...] = jnp.zeros(token_ref.shape, F32)
        for i in range(tiles):
            row = lax.broadcasted_iota(jnp.int32, (tile, size), 0)
            col = lax.broadcasted_iota(jnp.int32, (tile, size), 1)
            offset = col - row + (starts[i] - i * tile + BAND)
            offset = jnp.where(row + i * tile >= order_ref[0], offset, -1)
            odd = lax.rem(order_ref[0], 2)
            for d, shift in enumerate((2 - 2 * odd, 1, 2 * odd)):
                values = columns_ref[shift, i * tile : (i + 1) * tile, :]
                total = jnp.zeros((tile, size), F32)
                for k in range(width):
                    total = jnp.where(offset == k, values[:, k : k + 1], total)
                out_ref[d, i] = total.astype(BF16)

    return pl.pallas_call(
        kernel,
        in_specs=[
            pl.BlockSpec(memory_space=pltpu.SMEM),
            pl.BlockSpec(memory_space=pltpu.VMEM),
            pl.BlockSpec(memory_space=pltpu.HBM),
        ],
        out_specs=[pl.BlockSpec(memory_space=pltpu.VMEM)] * 2,
        out_shape=[
            jax.ShapeDtypeStruct((shifts, tiles, tile, size), BF16),
            jax.ShapeDtypeStruct((8, 128), F32),
        ],
        compiler_params=pltpu.CompilerParams(vmem_limit_bytes=ALL_VMEM),
        cost_estimate=pl.CostEstimate(
            flops=100_000_000, bytes_accessed=2_000_000, transcendentals=0
        ),
        name="bands",
    )(order.reshape(1), columns, after)


def coefficients(legendre, data, order, counts, after):
    degrees, nlat = legendre.shape
    tile = 256
    places = [(part, k) for part, count in enumerate(counts) for k in range(count // tile)]
    blocks = len(places)

    def kernel(order_ref, rows_hbm, data_hbm, *refs):
        outs = refs[len(after) : len(after) + len(counts)]
        rows_ref, data_ref, out_ref, sems, out_sems = refs[len(after) + len(counts) :]
        copies = [
            pltpu.make_async_copy(
                data_hbm.at[pl.ds(n * tile, tile)], data_ref.at[pl.ds(n * tile, tile)], sems.at[n + 1]
            )
            for n in range(blocks)
        ]
        rows_copy = pltpu.make_async_copy(rows_hbm, rows_ref, sems.at[0])
        copies[0].start()
        rows_copy.start()
        for copy in copies[1:]:
            copy.start()
        rows_copy.wait()
        sends = []
        for n, (part, k) in enumerate(places):
            copies[n].wait()
            coef = lax.dot_general(
                rows_ref[...],
                data_ref[n * tile : (n + 1) * tile, :],
                NT_DIMS,
                preferred_element_type=F32,
            )
            degree = lax.broadcasted_iota(jnp.int32, coef.shape, 0)
            out_ref[n] = jnp.where(degree >= order_ref[0], coef, 0.0).astype(BF16)
            cols = slice(k * tile, (k + 1) * tile)
            sends.append(
                pltpu.make_async_copy(out_ref.at[n], outs[part].at[:, cols], out_sems.at[n])
            )
            sends[n].start()
        for send in sends:
            send.wait()

    hbm = pl.BlockSpec(memory_space=pltpu.HBM)
    total = blocks * tile
    return pl.pallas_call(
        kernel,
        in_specs=[pl.BlockSpec(memory_space=pltpu.SMEM)] + [hbm] * (2 + len(after)),
        out_specs=[hbm] * len(counts),
        out_shape=[jax.ShapeDtypeStruct((degrees, count), BF16) for count in counts],
        scratch_shapes=[
            pltpu.VMEM((degrees, nlat), BF16),
            pltpu.VMEM((total, nlat), BF16),
            pltpu.VMEM((blocks, degrees, tile), BF16),
            pltpu.SemaphoreType.DMA((blocks + 1,)),
            pltpu.SemaphoreType.DMA((blocks,)),
        ],
        compiler_params=pltpu.CompilerParams(vmem_limit_bytes=ALL_VMEM),
        cost_estimate=pl.CostEstimate(
            flops=2 * degrees * nlat * total, bytes_accessed=2 * total * (nlat + degrees), transcendentals=0
        ),
        name="coef",
    )(order.reshape(1), legendre, data, *after)


def deconvolve(near, here, far, bands, wtable, first, last, parts, turn):
    degrees, count = here.shape
    half = wtable.shape[1]
    shifts, tiles, tile, size = bands.shape
    _, starts = windows(degrees, tile, (size - tile) // 2)
    block, strip = 256, 256

    def kernel(near_ref, here_ref, far_ref, bands_ref, wtable_ref, *refs):
        sources = (near_ref, here_ref, far_ref)
        mixed_ref = refs[4] if last else refs[-1]
        for i in range(tiles):
            for n in range(count // strip):
                cols = slice(n * strip, (n + 1) * strip)
                acc = jnp.zeros((tile, strip), F32)
                for d in range(shifts):
                    acc += jnp.dot(
                        bands_ref[d, i],
                        sources[d][starts[i] : starts[i] + size, cols],
                        preferred_element_type=F32,
                    )
                mixed_ref[i * tile : (i + 1) * tile, cols] = acc.astype(BF16)

        def transform(cols):
            return jnp.dot(
                mixed_ref[...],
                wtable_ref[first : first + count, cols],
                preferred_element_type=F32,
            )

        if not last:
            for n in range(half // block):
                cols = slice(n * block, (n + 1) * block)
                refs[-2][:, cols] = transform(cols)
            return
        even_ref, odd_ref, turn_ref, out_ref, _, stage_ref, sems = refs
        copies = []
        quarter = half // 2
        for n in range(quarter // block):
            real = slice(n * block, (n + 1) * block)
            imag = slice(quarter + n * block, quarter + (n + 1) * block)
            odd_real = transform(real) + odd_ref[:, real]
            odd_imag = transform(imag) + odd_ref[:, imag]
            cosine = turn_ref[0:1, real]
            sine = turn_ref[1:2, real]
            turned_real = cosine * odd_real + sine * odd_imag
            turned_imag = cosine * odd_imag - sine * odd_real
            results = (
                even_ref[:, real] + turned_real,
                even_ref[:, real] - turned_real,
                even_ref[:, imag] + turned_imag,
                even_ref[:, imag] - turned_imag,
            )
            for k, result in enumerate(results):
                slot = 4 * n + k
                at = k * quarter + n * block
                stage_ref[slot] = result
                copies.append(
                    pltpu.make_async_copy(
                        stage_ref.at[slot], out_ref.at[:, at : at + block], sems.at[slot]
                    )
                )
                copies[-1].start()
        for copy in copies:
            copy.wait()

    vmem = pl.BlockSpec(memory_space=pltpu.VMEM)
    scratch = [pltpu.VMEM((degrees, count), BF16)]
    inputs = [near, here, far, bands, wtable]
    if last:
        slots = 2 * half // block
        scratch += [pltpu.VMEM((slots, degrees, block), F32), pltpu.SemaphoreType.DMA((slots,))]
        parts = [*parts, turn]
    inputs += parts
    return pl.pallas_call(
        kernel,
        in_specs=[vmem] * len(inputs),
        out_specs=pl.BlockSpec(memory_space=pltpu.HBM) if last else vmem,
        out_shape=jax.ShapeDtypeStruct((degrees, 2 * half if last else half), F32),
        scratch_shapes=scratch,
        compiler_params=pltpu.CompilerParams(vmem_limit_bytes=16 * MIB),
        cost_estimate=pl.CostEstimate(
            flops=2 * degrees * count * half, bytes_accessed=20_000_000, transcendentals=0
        ),
        name="last" if last else "deconvolve",
    )(*inputs)


def on_device(images, legendre, leakage):
    devices = lax.axis_size("dev")
    order = lax.axis_index("dev").astype(jnp.int32)
    tloc, nlat, _ = images.shape
    mates = [(i, i ^ 1) for i in range(devices)]
    across = [(i, i - 1 + 2 * (i % 2)) for i in range(1, devices - 1)]
    data, after = [], ()
    for group in range(GROUPS):
        sent = transform_images(images, devices, group, after)
        gathered = lax.all_to_all(sent, "dev", split_axis=0, concat_axis=0, tiled=True)
        data.append(gathered.reshape(-1, nlat))
        if group == 0:
            bands, token = band_matrices(leakage[0], order, 176, 16, sent)
            after = (token,)
    parts, after = [], ()
    for group, counts in enumerate(CHUNKS):
        coefs = coefficients(legendre[0], data[group], order, counts, after)
        for coef in coefs:
            far = lax.ppermute(coef, "dev", across)
            near = lax.ppermute(coef, "dev", mates)
            parts.append((near, coef, far))
        if group == 0:
            table, token = time_matrix(devices, tloc, coefs[0])
            after = (token,)
    turn = jnp.asarray(time_factors(devices, tloc)[2])
    sums = []
    for (first, final), part in zip(PLACES, parts):
        sums.append(deconvolve(*part, bands, table, first, final, sums, turn))
    return sums[-1][None]


def solution(mesh):
    placed = (P("dev", None, None), P("dev", None, None), P("dev", None, None, None))
    return jax.shard_map(
        on_device, mesh=mesh, in_specs=placed, out_specs=P("dev", None, None), check_vma=False
    )
```

```python
import math

import jax
import jax.numpy as jnp
import numpy as np
from jax import lax
from jax.experimental import pallas as pl
from jax.experimental.pallas import tpu as pltpu
from jax.sharding import PartitionSpec as P

BAND = 6
F32 = jnp.float32
BF16 = jnp.bfloat16
MIB = 1 << 20
ALL_VMEM = 67_000_000
GROUPS = 2
CHUNKS = ((1024,), (768, 256))
PLACES = ((0, False), (0, False), (768, True))
NT_DIMS = (((1,), (1,)), ((), ()))


def lon_table(nlon, norders):
    phase = (np.arange(nlon)[:, None] * np.arange(norders)[None, :]) % nlon
    angle = 2.0 * math.pi * phase / nlon
    table = np.concatenate([np.cos(angle), -np.sin(angle)], axis=1) / math.sqrt(nlon)
    return table.astype(BF16)


def time_factors(nsrc, tloc):
    half = nsrc * tloc // 2
    per = tloc // GROUPS
    slow = 2.0 * math.pi * ((np.arange(nsrc)[:, None] * np.arange(128)[None, :]) % nsrc) / nsrc
    fast = 2.0 * math.pi * ((np.arange(per)[:, None] * np.arange(half)[None, :]) % half) / half
    slow = np.stack([np.cos(slow), np.sin(slow)]) / math.sqrt(2 * half)
    plain = np.stack([np.cos(fast), np.sin(fast)], axis=1).reshape(2 * per, half)
    turned = np.stack([-np.sin(fast), np.cos(fast)], axis=1).reshape(2 * per, half)
    turn = math.pi * np.arange(half) / half
    turn = np.stack([np.cos(turn), np.sin(turn)])
    return [x.astype(np.float32) for x in (slow, np.stack([plain, turned]), turn)]


def transform_images(images, norders, group, after):
    tloc, nlat, nlon = images.shape
    per = tloc // GROUPS
    tile, some = 384, 8
    rows = 2 * norders

    def kernel(table_ref, image_ref, *refs):
        out_ref, turned_ref = refs[-2:]
        flat = image_ref[...].reshape(per * tile, nlon)
        part = jnp.dot(flat, table_ref[...], preferred_element_type=F32)
        for t in range(per):
            turned_ref[2 * t : 2 * t + 2] = part[t * tile : (t + 1) * tile].T.reshape(2, norders, tile)
        for i in range(0, norders, some):
            swapped = jnp.swapaxes(turned_ref[:, i : i + some, :], 0, 1)
            out_ref[i : i + some] = swapped.astype(BF16)

    return pl.pallas_call(
        kernel,
        grid=(nlat // tile,),
        in_specs=[
            pl.BlockSpec((nlon, rows), lambda j: (0, 0)),
            pl.BlockSpec((per, None, tile, nlon), lambda j: (0, group, j, 0)),
        ]
        + [pl.BlockSpec(memory_space=pltpu.HBM)] * len(after),
        out_specs=pl.BlockSpec((norders, 2 * per, tile), lambda j: (0, 0, j)),
        out_shape=jax.ShapeDtypeStruct((norders, 2 * per, nlat), BF16),
        scratch_shapes=[pltpu.VMEM((2 * per, norders, tile), F32)],
        compiler_params=pltpu.CompilerParams(vmem_limit_bytes=ALL_VMEM),
        cost_estimate=pl.CostEstimate(
            flops=2 * rows * per * nlat * nlon, bytes_accessed=images.size * 2, transcendentals=0
        ),
        name="lon",
    )(jnp.asarray(lon_table(nlon, norders)), images.reshape(per, GROUPS, nlat, nlon), *after)


def time_matrix(nsrc, tloc, after):
    ntimes = nsrc * tloc // 2
    slow, fast, _ = time_factors(nsrc, tloc)
    rows = 2 * tloc // GROUPS
    per = 32
    lanes = 128
    count = nsrc * rows

    def kernel(slow_ref, fast_ref, after_ref, out_ref, token_ref):
        token_ref[...] = jnp.zeros(token_ref.shape, F32)

        def sources(s, carry):
            a = [slow_ref[0, pl.ds(2 * s + u, 1), :] for u in range(2)]
            b = [slow_ref[1, pl.ds(2 * s + u, 1), :] for u in range(2)]
            here = pl.ds(pl.multiple_of(s * 2 * rows, 2 * rows), 2 * rows)
            for f in range(ntimes // lanes):
                cols = slice(f * lanes, (f + 1) * lanes)
                more = slice(ntimes + f * lanes, ntimes + (f + 1) * lanes)
                plain = fast_ref[0, :, cols]
                turned = fast_ref[1, :, cols]
                left = [a[u] * plain + b[u] * turned for u in range(2)]
                right = [a[u] * turned - b[u] * plain for u in range(2)]
                out_ref[here, cols] = jnp.concatenate(left, axis=0).astype(BF16)
                out_ref[here, more] = jnp.concatenate(right, axis=0).astype(BF16)
            return carry

        lax.fori_loop(0, per // 2, sources, 0)

    return pl.pallas_call(
        kernel,
        grid=(count // rows // per,),
        in_specs=[
            pl.BlockSpec((2, per, lanes), lambda i: (0, i, 0)),
            pl.BlockSpec((2, rows, ntimes), lambda i: (0, 0, 0)),
            pl.BlockSpec(memory_space=pltpu.HBM),
        ],
        out_specs=[
            pl.BlockSpec((per * rows, 2 * ntimes), lambda i: (i, 0)),
            pl.BlockSpec((8, lanes), lambda i: (0, 0)),
        ],
        out_shape=[
            jax.ShapeDtypeStruct((count, 2 * ntimes), BF16),
            jax.ShapeDtypeStruct((8, lanes), F32),
        ],
        compiler_params=pltpu.CompilerParams(vmem_limit_bytes=ALL_VMEM),
        cost_estimate=pl.CostEstimate(
            flops=100_000_000, bytes_accessed=4 * ntimes * count, transcendentals=0
        ),
        name="time_matrix",
    )(jnp.asarray(slow), jnp.asarray(fast), after)


def windows(degrees, tile, reach):
    size = tile + 2 * reach
    return size, [min(max(i * tile - reach, 0), degrees - size) for i in range(degrees // tile)]


def band_matrices(leakage, order, tile, reach, after):
    shifts, width, degrees = leakage.shape
    size, starts = windows(degrees, tile, reach)
    tiles = degrees // tile
    columns = jnp.transpose(leakage, (0, 2, 1))

    def kernel(order_ref, columns_ref, after_ref, out_ref, token_ref):
        token_ref[...] = jnp.zeros(token_ref.shape, F32)
        for i in range(tiles):
            row = lax.broadcasted_iota(jnp.int32, (tile, size), 0)
            col = lax.broadcasted_iota(jnp.int32, (tile, size), 1)
            offset = col - row + (starts[i] - i * tile + BAND)
            offset = jnp.where(row + i * tile >= order_ref[0], offset, -1)
            odd = lax.rem(order_ref[0], 2)
            for d, shift in enumerate((2 - 2 * odd, 1, 2 * odd)):
                values = columns_ref[shift, i * tile : (i + 1) * tile, :]
                total = jnp.zeros((tile, size), F32)
                for k in range(width):
                    total = jnp.where(offset == k, values[:, k : k + 1], total)
                out_ref[d, i] = total.astype(BF16)

    return pl.pallas_call(
        kernel,
        in_specs=[
            pl.BlockSpec(memory_space=pltpu.SMEM),
            pl.BlockSpec(memory_space=pltpu.VMEM),
            pl.BlockSpec(memory_space=pltpu.HBM),
        ],
        out_specs=[pl.BlockSpec(memory_space=pltpu.VMEM)] * 2,
        out_shape=[
            jax.ShapeDtypeStruct((shifts, tiles, tile, size), BF16),
            jax.ShapeDtypeStruct((8, 128), F32),
        ],
        compiler_params=pltpu.CompilerParams(vmem_limit_bytes=ALL_VMEM),
        cost_estimate=pl.CostEstimate(
            flops=100_000_000, bytes_accessed=2_000_000, transcendentals=0
        ),
        name="bands",
    )(order.reshape(1), columns, after)


def coefficients(legendre, data, order, counts, after):
    degrees, nlat = legendre.shape
    tile = 256
    places = [(part, k) for part, count in enumerate(counts) for k in range(count // tile)]
    blocks = len(places)

    def kernel(order_ref, rows_hbm, data_hbm, *refs):
        outs = refs[len(after) : len(after) + len(counts)]
        rows_ref, data_ref, out_ref, sems, out_sems = refs[len(after) + len(counts) :]
        copies = [
            pltpu.make_async_copy(
                data_hbm.at[pl.ds(n * tile, tile)], data_ref.at[pl.ds(n * tile, tile)], sems.at[n + 1]
            )
            for n in range(blocks)
        ]
        rows_copy = pltpu.make_async_copy(rows_hbm, rows_ref, sems.at[0])
        copies[0].start()
        rows_copy.start()
        for copy in copies[1:]:
            copy.start()
        rows_copy.wait()
        sends = []
        for n, (part, k) in enumerate(places):
            copies[n].wait()
            coef = lax.dot_general(
                rows_ref[...],
                data_ref[n * tile : (n + 1) * tile, :],
                NT_DIMS,
                preferred_element_type=F32,
            )
            degree = lax.broadcasted_iota(jnp.int32, coef.shape, 0)
            out_ref[n] = jnp.where(degree >= order_ref[0], coef, 0.0).astype(BF16)
            cols = slice(k * tile, (k + 1) * tile)
            sends.append(
                pltpu.make_async_copy(out_ref.at[n], outs[part].at[:, cols], out_sems.at[n])
            )
            sends[n].start()
        for send in sends:
            send.wait()

    hbm = pl.BlockSpec(memory_space=pltpu.HBM)
    total = blocks * tile
    return pl.pallas_call(
        kernel,
        in_specs=[pl.BlockSpec(memory_space=pltpu.SMEM)] + [hbm] * (2 + len(after)),
        out_specs=[hbm] * len(counts),
        out_shape=[jax.ShapeDtypeStruct((degrees, count), BF16) for count in counts],
        scratch_shapes=[
            pltpu.VMEM((degrees, nlat), BF16),
            pltpu.VMEM((total, nlat), BF16),
            pltpu.VMEM((blocks, degrees, tile), BF16),
            pltpu.SemaphoreType.DMA((blocks + 1,)),
            pltpu.SemaphoreType.DMA((blocks,)),
        ],
        compiler_params=pltpu.CompilerParams(vmem_limit_bytes=ALL_VMEM),
        cost_estimate=pl.CostEstimate(
            flops=2 * degrees * nlat * total, bytes_accessed=2 * total * (nlat + degrees), transcendentals=0
        ),
        name="coef",
    )(order.reshape(1), legendre, data, *after)


def deconvolve(near, here, far, bands, wtable, first, last, parts, turn):
    degrees, count = here.shape
    half = wtable.shape[1]
    shifts, tiles, tile, size = bands.shape
    _, starts = windows(degrees, tile, (size - tile) // 2)
    block, strip = 128 if last else 256, 256

    def kernel(near_ref, here_ref, far_ref, bands_ref, wtable_ref, *refs):
        sources = (near_ref, here_ref, far_ref)
        mixed_ref = refs[4] if last else refs[-1]
        for i in range(tiles):
            for n in range(count // strip):
                cols = slice(n * strip, (n + 1) * strip)
                acc = jnp.zeros((tile, strip), F32)
                for d in range(shifts):
                    acc += jnp.dot(
                        bands_ref[d, i],
                        sources[d][starts[i] : starts[i] + size, cols],
                        preferred_element_type=F32,
                    )
                mixed_ref[i * tile : (i + 1) * tile, cols] = acc.astype(BF16)

        def transform(cols):
            return jnp.dot(
                mixed_ref[...],
                wtable_ref[first : first + count, cols],
                preferred_element_type=F32,
            )

        if not last:
            for n in range(half // block):
                cols = slice(n * block, (n + 1) * block)
                refs[-2][:, cols] = transform(cols)
            return
        even_ref, odd_ref, turn_ref, out_ref, _, stage_ref, sems = refs
        copies = []
        quarter = half // 2
        for n in range(quarter // block):
            real = slice(n * block, (n + 1) * block)
            imag = slice(quarter + n * block, quarter + (n + 1) * block)
            odd_real = transform(real) + odd_ref[:, real]
            odd_imag = transform(imag) + odd_ref[:, imag]
            cosine = turn_ref[0:1, real]
            sine = turn_ref[1:2, real]
            turned_real = cosine * odd_real + sine * odd_imag
            turned_imag = cosine * odd_imag - sine * odd_real
            results = (
                even_ref[:, real] + turned_real,
                even_ref[:, real] - turned_real,
                even_ref[:, imag] + turned_imag,
                even_ref[:, imag] - turned_imag,
            )
            for k, result in enumerate(results):
                slot = 4 * n + k
                at = k * quarter + n * block
                stage_ref[slot] = result
                copies.append(
                    pltpu.make_async_copy(
                        stage_ref.at[slot], out_ref.at[:, at : at + block], sems.at[slot]
                    )
                )
                copies[-1].start()
        for copy in copies:
            copy.wait()

    vmem = pl.BlockSpec(memory_space=pltpu.VMEM)
    scratch = [pltpu.VMEM((degrees, count), BF16)]
    inputs = [near, here, far, bands, wtable]
    if last:
        slots = 2 * half // block
        scratch += [pltpu.VMEM((slots, degrees, block), F32), pltpu.SemaphoreType.DMA((slots,))]
        parts = [*parts, turn]
    inputs += parts
    return pl.pallas_call(
        kernel,
        in_specs=[vmem] * len(inputs),
        out_specs=pl.BlockSpec(memory_space=pltpu.HBM) if last else vmem,
        out_shape=jax.ShapeDtypeStruct((degrees, 2 * half if last else half), F32),
        scratch_shapes=scratch,
        compiler_params=pltpu.CompilerParams(vmem_limit_bytes=16 * MIB),
        cost_estimate=pl.CostEstimate(
            flops=2 * degrees * count * half, bytes_accessed=20_000_000, transcendentals=0
        ),
        name="last" if last else "deconvolve",
    )(*inputs)


def on_device(images, legendre, leakage):
    devices = lax.axis_size("dev")
    order = lax.axis_index("dev").astype(jnp.int32)
    tloc, nlat, _ = images.shape
    mates = [(i, i ^ 1) for i in range(devices)]
    across = [(i, i - 1 + 2 * (i % 2)) for i in range(1, devices - 1)]
    data, after = [], ()
    for group in range(GROUPS):
        sent = transform_images(images, devices, group, after)
        gathered = lax.all_to_all(sent, "dev", split_axis=0, concat_axis=0, tiled=True)
        data.append(gathered.reshape(-1, nlat))
        if group == 0:
            bands, token = band_matrices(leakage[0], order, 176, 16, sent)
            after = (token,)
    parts, after = [], ()
    for group, counts in enumerate(CHUNKS):
        coefs = coefficients(legendre[0], data[group], order, counts, after)
        for coef in coefs:
            far = lax.ppermute(coef, "dev", across)
            near = lax.ppermute(coef, "dev", mates)
            parts.append((near, coef, far))
        if group == 0:
            table, token = time_matrix(devices, tloc, coefs[0])
            after = (token,)
    turn = jnp.asarray(time_factors(devices, tloc)[2])
    sums = []
    for (first, final), part in zip(PLACES, parts):
        sums.append(deconvolve(*part, bands, table, first, final, sums, turn))
    return sums[-1][None]


def solution(mesh):
    placed = (P("dev", None, None), P("dev", None, None), P("dev", None, None, None))
    return jax.shard_map(
        on_device, mesh=mesh, in_specs=placed, out_specs=P("dev", None, None), check_vma=False
    )
```
